32 devices in a mesh: bvec: 4 (over y, x), row: 2 (over core), col: 4 (over z).
Axes of the slice: x: 2, y: 2, z: 4, core: 2. Of those that a mesh axis runs over, the one named last changes fastest.
Arguments:
- m_matrices: float32 [4, 2, 2048, 2048], P('bvec', None, 'row', 'col'), may hold values from -2 to 2, as said below
- bvec_index: int32 [4], replicated, may hold values from 0 to 5
- weight_table: float32 [6], replicated, may hold values from 0.25 to 2
- grad_prev: float32 [2048, 2048], P('row', 'col'), may hold values from -4 to 4, as said below
- dir_prev: float32 [2048, 2048], P('row', 'col'), may hold values from -4 to 4, as said below
Outputs:
- spread: float32 [], replicated
- trial_spread: float32 [], replicated
- gradient: float32 [2048, 2048], P('row', 'col')
- direction: float32 [2048, 2048], P('row', 'col')
- trial_diag: float32 [4, 2, 2048], replicated
The draws below stay inside these ranges and needn't reach their ends.
Inputs may be any that keep to these rules, and one draw needn't show every extreme that they name: Each matrix m_matrices[b, p] is symmetric. grad_prev is antisymmetric. dir_prev is antisymmetric.
All inputs are finite; a program needn't handle non-finite values.
Results may differ from the reference program's by a relative error of at most 0.0003.
Values sent between devices are 32-bit elements; how exact they have to be, the bound alone decides.
A program may use at most 128 MiB of HBM per device.

```python
import math
import jax
import jax.numpy as jnp
from jax import lax

N = 2048
NTAB = 6
TAYLOR = 8
NB = 4


def draw_m_matrices(key, part):
    subkeys = jax.random.split(jax.random.fold_in(key, 101), 4)
    gaussian = jax.random.normal(subkeys[0], (NB, 2, N, N), jnp.float32)
    noise_scale = 0.25
    radius = jax.random.uniform(subkeys[1], (NB, N), jnp.float32, 0.3, 0.95)
    angles = jax.random.uniform(subkeys[2], (NB, N), jnp.float32, -math.pi, math.pi)
    symmetric = (gaussian + jnp.swapaxes(gaussian, 2, 3)) * (noise_scale / math.sqrt(2.0))
    identity = jnp.eye(N, dtype=jnp.float32)
    diag_parts = jnp.stack([radius * jnp.cos(angles), radius * jnp.sin(angles)], axis=1)
    matrix = symmetric * (1.0 - identity) + diag_parts[:, :, :, None] * identity
    return jnp.clip(matrix, -2.0, 2.0)


def antisymmetric(key, noise_scale):
    gaussian = jax.random.normal(key, (N, N), jnp.float32)
    factor = noise_scale
    return jnp.clip((gaussian - gaussian.T) * (factor / math.sqrt(2.0)), -4.0, 4.0)


def draw_grad_prev(key, part):
    return antisymmetric(jax.random.fold_in(key, 7), 0.6)


def draw_dir_prev(key, part):
    return antisymmetric(jax.random.fold_in(key, 13), 0.6)


def plant(array, rng, smallest, top_value):
    spot = [jax.random.randint(jax.random.fold_in(rng, axis), (), 0, length) for axis, length in enumerate(array.shape)]
    longest = array.shape.index(max(array.shape))
    neighbour = spot[:longest] + [(spot[longest] + 1) % array.shape[longest]] + spot[longest + 1:]
    return array.at[tuple(spot)].set(smallest).at[tuple(neighbour)].set(top_value)


def setup_inputs(seed: int = 0) -> dict:
    seeds = jax.random.split(jax.random.key(seed), 6)
    return {
        "m_matrices": draw_m_matrices(jax.random.fold_in(seeds[5], 71), 0),
        "bvec_index": plant(jax.random.randint(seeds[1], (NB,), 0, NTAB), jax.random.fold_in(seeds[1], 1), 0, NTAB - 1).astype(jnp.int32),
        "weight_table": jnp.clip(jnp.exp(jax.random.uniform(seeds[2], (NTAB,), jnp.float32, math.log(0.25), math.log(2.0))), 0.25, 2.0),
        "grad_prev": draw_grad_prev(jax.random.fold_in(seeds[5], 71), 0),
        "dir_prev": draw_dir_prev(jax.random.fold_in(seeds[5], 71), 0),
    }


def product(left, right):
    return jnp.dot(left, right, precision=lax.Precision.HIGHEST, preferred_element_type=jnp.float32)

def reference(m_matrices, bvec_index, weight_table, grad_prev, dir_prev):
    table_slots = jnp.arange(weight_table.shape[0], dtype=jnp.int32)
    weight = lax.optimization_barrier(jnp.sum(jnp.where(table_slots[None, :] == bvec_index[:, None], weight_table[None, :], 0.0), axis=1))
    re_diag = jnp.diagonal(m_matrices[:, 0], axis1=1, axis2=2)
    im_diag = jnp.diagonal(m_matrices[:, 1], axis1=1, axis2=2)
    spread = jnp.sum(weight[:, None] * (1.0 - re_diag ** 2 - im_diag ** 2)) / N
    gradient = jnp.zeros((N, N), jnp.float32)
    for bvec in range(NB):
        real_term = m_matrices[bvec, 0] * (re_diag[bvec][:, None] - re_diag[bvec][None, :])
        imag_term = m_matrices[bvec, 1] * (im_diag[bvec][:, None] - im_diag[bvec][None, :])
        gradient = gradient + 2.0 * weight[bvec] * (real_term + imag_term)
    beta_factor = jnp.sum(gradient * gradient) / (1.0 + jnp.sum(grad_prev * grad_prev))
    direction = beta_factor * dir_prev - gradient
    trial_generator = 1.75 * direction / jnp.sqrt(1.0 + jnp.sum(direction * direction) / N)
    identity = jnp.eye(N, dtype=jnp.float32)
    horner = identity + trial_generator / TAYLOR
    for degree in range(TAYLOR - 1, 0, -1):
        horner = identity + product(horner, trial_generator) / degree
    expmap = horner
    entries = []
    for bvec in range(NB):
        parts = []
        for index in range(2):
            rotated = product(m_matrices[bvec, index], expmap)
            parts.append(lax.optimization_barrier(jnp.sum(expmap * rotated, axis=0)))
        entries.append(jnp.stack(parts, axis=0))
    trial_diag = jnp.stack(entries, axis=0)
    trial_spread = jnp.sum(weight[:, None] * (1.0 - trial_diag[:, 0] ** 2 - trial_diag[:, 1] ** 2)) / N
    return (spread, trial_spread, gradient, direction, trial_diag)
```

```python
import jax
import jax.numpy as jnp
from jax import lax
from jax.sharding import PartitionSpec as P

TAYLOR = 8
STEP_SCALE = 1.75
HIGH = lax.Precision.HIGH
ALL = ("bvec", "row", "col")


def product(left, right):
    return jnp.dot(left, right, precision=HIGH, preferred_element_type=jnp.float32)


def lookup_weights(bvec_index, weight_table):
    table_slots = jnp.arange(weight_table.shape[0], dtype=jnp.int32)
    return jnp.sum(
        jnp.where(table_slots[None, :] == bvec_index[:, None], weight_table[None, :], 0.0), axis=1
    )


def shards(m_matrices, bvec_index, weight_table, grad_prev, dir_prev):
    per_group = m_matrices.shape[0]
    local_rows = m_matrices.shape[2]
    local_cols = m_matrices.shape[3]
    groups, n_row, n_col = (lax.axis_size(a) for a in ALL)
    devices = groups * n_row * n_col
    order = local_rows * n_row
    group = lax.axis_index("bvec")
    row, col = lax.axis_index("row"), lax.axis_index("col")
    row_start = row * local_rows
    col_start = col * local_cols
    weight_all = lookup_weights(bvec_index, weight_table)
    weight_own = lax.dynamic_slice_in_dim(weight_all, group * per_group, per_group)
    row_ids = row_start + jnp.arange(local_rows, dtype=jnp.int32)
    col_ids = col_start + jnp.arange(local_cols, dtype=jnp.int32)
    on_diag = row_ids[:, None] == col_ids[None, :]
    own_diag = jnp.sum(jnp.where(on_diag, m_matrices, 0.0), axis=2)
    diag_parts = lax.all_gather(own_diag, ("row", "col"))
    diag_parts = diag_parts.reshape(n_row, n_col, per_group, 2, local_cols).sum(axis=0)
    diagonal = diag_parts.transpose(1, 2, 0, 3).reshape(per_group, 2, order)
    row_diag = lax.dynamic_slice_in_dim(diagonal, row_start, local_rows, 2)
    col_diag = lax.dynamic_slice_in_dim(diagonal, col_start, local_cols, 2)
    spread_own = (
        jnp.sum(weight_own[:, None] * (1.0 - diagonal[:, 0] ** 2 - diagonal[:, 1] ** 2)) / order
    )
    spread_term = jnp.where((row == 0) & (col == 0), spread_own, 0.0)
    differ = row_diag[:, :, :, None] - col_diag[:, :, None, :]
    weighted = 2.0 * weight_own[:, None, None] * jnp.sum(m_matrices * differ, axis=1)
    grad_part = jnp.sum(weighted, axis=0)
    grad_piece = lax.psum_scatter(grad_part, "bvec", scatter_dimension=0, tiled=True)
    piece_rows = local_rows // groups
    prev_piece = lax.dynamic_slice_in_dim(grad_prev, group * piece_rows, piece_rows, 0)
    dir_piece = lax.dynamic_slice_in_dim(dir_prev, group * piece_rows, piece_rows, 0)
    sums = jnp.stack(
        [
            spread_term,
            jnp.sum(grad_piece * grad_piece),
            jnp.sum(prev_piece * prev_piece),
            jnp.sum(grad_piece * dir_piece),
            jnp.sum(dir_piece * dir_piece),
        ]
    )
    totals = jnp.sum(lax.all_gather(sums, ALL), axis=0)
    spread = totals[0]
    beta_factor = totals[1] / (1.0 + totals[2])
    dir_norm = jnp.maximum(
        totals[1] - 2.0 * beta_factor * totals[3] + beta_factor * beta_factor * totals[4], 0.0
    )
    scale = STEP_SCALE / jnp.sqrt(1.0 + dir_norm / order)
    x_piece = scale * (beta_factor * dir_piece - grad_piece)
    pieces = lax.all_gather(x_piece, ALL)
    grad_in, _ = lax.optimization_barrier((grad_piece, pieces[0, 0, 0]))
    gradient = lax.all_gather(grad_in, "bvec", axis=0, tiled=True)
    direction = beta_factor * dir_prev - gradient

    whole = pieces.reshape(groups, n_row, n_col, piece_rows, local_cols)
    generator = whole.transpose(1, 0, 3, 2, 4).reshape(order, order)
    slab = order // devices
    me = (group * n_row + row) * n_col + col
    slab_ids = me * slab + jnp.arange(slab, dtype=jnp.int32)
    eye_slab = (slab_ids[:, None] == jnp.arange(order, dtype=jnp.int32)[None, :]).astype(jnp.float32)
    iterate = eye_slab + lax.dynamic_slice_in_dim(generator, me * slab, slab, 0) / TAYLOR
    for divisor in range(TAYLOR - 1, 0, -1):
        iterate = eye_slab + product(iterate, generator) / divisor
    expmap = lax.all_gather(iterate, ALL, axis=0, tiled=True)
    exp_rows = lax.dynamic_slice_in_dim(expmap, row_start, local_rows, 0)
    exp_cols = lax.dynamic_slice_in_dim(expmap, col_start, local_cols, 0)
    flat = m_matrices.reshape(-1, local_cols)
    rotated = product(flat, exp_cols).reshape(per_group, 2, local_rows, order)
    trial_part = jnp.sum(exp_rows[None, None] * rotated, axis=2)
    trial_parts = lax.all_gather(trial_part, ALL)
    trial_diag = trial_parts.reshape(groups, n_row * n_col, per_group, 2, order).sum(axis=1)
    trial_diag = trial_diag.reshape(groups * per_group, 2, order)
    trial_spread = (
        jnp.sum(weight_all[:, None] * (1.0 - trial_diag[:, 0] ** 2 - trial_diag[:, 1] ** 2)) / order
    )
    return (spread, trial_spread, gradient, direction, trial_diag)


def solution(mesh):
    placed = (P("bvec", None, "row", "col"), P(), P(), P("row", "col"), P("row", "col"))
    return jax.shard_map(
        shards,
        mesh=mesh,
        in_specs=placed,
        out_specs=(P(), P(), P("row", "col"), P("row", "col"), P()),
        check_vma=False,
    )
```

```python
import jax
import jax.numpy as jnp
from jax import lax
from jax.experimental import pallas as pl
from jax.experimental.pallas import tpu as pltpu
from jax.sharding import PartitionSpec as P

TAYLOR = 8
STEP_SCALE = 1.75
HIGH = lax.Precision.HIGH
ALL = ("bvec", "row", "col")


def product(left, right):
    return jnp.dot(left, right, precision=HIGH, preferred_element_type=jnp.float32)


def member(position, axes, sizes):
    where = {}
    for axis, size in zip(reversed(axes), reversed(sizes)):
        where[axis] = lax.rem(position, size)
        position = lax.div(position, size)
    return where


def small_gather(block, axes, collective_id):
    sizes = tuple(lax.axis_size(axis) for axis in axes)
    count = 1
    for size in sizes:
        count *= size
    if count > 32:
        return lax.all_gather(block, axes)

    def kernel(block_ref, out_ref, send_sem, recv_sem, local_sem):
        me = lax.axis_index(axes[0])
        for axis, size in zip(axes[1:], sizes[1:]):
            me = me * size + lax.axis_index(axis)
        barrier = pltpu.get_barrier_semaphore()

        def peer(step):
            return member(lax.rem(me + step, count), axes, sizes)

        def greet(step, carry):
            pl.semaphore_signal(
                barrier, inc=1, device_id=peer(step), device_id_type=pl.DeviceIdType.MESH
            )
            return carry

        def copy(step):
            return pltpu.make_async_remote_copy(
                src_ref=block_ref,
                dst_ref=out_ref.at[me],
                send_sem=send_sem.at[step],
                recv_sem=recv_sem.at[step],
                device_id=peer(step),
                device_id_type=pl.DeviceIdType.MESH,
            )

        def start(step, carry):
            copy(step).start()
            return carry

        def finish(step, carry):
            copy(step).wait()
            return carry

        own = pltpu.make_async_copy(block_ref, out_ref.at[me], local_sem)
        own.start()
        lax.fori_loop(1, count, greet, 0)
        pl.semaphore_wait(barrier, count - 1)
        lax.fori_loop(1, count, start, 0)
        lax.fori_loop(1, count, finish, 0)
        own.wait()

    return pl.pallas_call(
        kernel,
        out_shape=jax.ShapeDtypeStruct((count,) + block.shape, block.dtype),
        in_specs=[pl.BlockSpec(memory_space=pltpu.VMEM)],
        out_specs=pl.BlockSpec(memory_space=pltpu.VMEM),
        scratch_shapes=[
            pltpu.SemaphoreType.DMA((count,)),
            pltpu.SemaphoreType.DMA((count,)),
            pltpu.SemaphoreType.DMA,
        ],
        compiler_params=pltpu.CompilerParams(collective_id=collective_id, has_side_effects=True),
    )(block)


def wide_gather(piece, shape, place, band, collective_id):
    quarter = piece.shape[0] // 4
    first, second = (0, 2 * quarter), (2 * quarter, 2 * quarter)
    quarters = [(i * quarter, quarter) for i in range(4)]

    def kernel(piece_ref, out_ref, send_sem, recv_sem, local_sem):
        g, r, c = (lax.axis_index(a) for a in ALL)
        gx, gy = g + 1 - 2 * lax.rem(g, 2), lax.rem(g + 2, 4)
        gd = lax.rem(gx + 2, 4)
        cp, cm, c2 = lax.rem(c + 1, 4), lax.rem(c + 3, 4), lax.rem(c + 2, 4)
        to_x, to_y = {"bvec": gx}, {"bvec": gy}
        to_p, to_m = {"col": cp}, {"col": cm}
        to_core = {"row": 1 - r}
        started = []

        def send(source, target, peer):
            k = len(started)
            copy = pltpu.make_async_remote_copy(
                src_ref=source,
                dst_ref=target,
                send_sem=send_sem.at[k],
                recv_sem=recv_sem.at[k],
                device_id=peer,
                device_id_type=pl.DeviceIdType.MESH,
            )
            copy.start()
            started.append(copy)
            return copy

        def own(part, peer):
            return send(piece_ref.at[pl.ds(*part)], place(out_ref, g, r, c, part), peer)

        def pass_on(gg, cc, part, peer):
            spot = place(out_ref, gg, r, cc, part)
            return send(spot, spot, peer)

        def share(gg, part):
            spot = band(out_ref, gg, r, part)
            return send(spot, spot, to_core)

        barrier = pltpu.get_barrier_semaphore()
        for peer in (to_x, to_y, to_p, to_m, to_core):
            pl.semaphore_signal(barrier, inc=1, device_id=peer, device_id_type=pl.DeviceIdType.MESH)
        pl.semaphore_wait(barrier, 5)
        a_p, a_m = own(first, to_p), own(first, to_m)
        b_x, b_y = own(second, to_x), own(second, to_y)
        ax, ay, bp, bm = {}, {}, {}, {}
        ax[0], ay[0] = own(first, to_x), own(first, to_y)
        bp[0], bm[0] = own(second, to_p), own(second, to_m)
        local = pltpu.make_async_copy(
            piece_ref, place(out_ref, g, r, c, (0, 4 * quarter)), local_sem
        )
        local.start()
        a_p.wait_recv()
        relay_p = pass_on(g, cm, quarters[0], to_p)
        b_x.wait_recv()
        relay_y = pass_on(gx, c, quarters[2], to_y)
        a_m.wait_recv()
        relay_m = pass_on(g, cp, quarters[1], to_m)
        b_y.wait_recv()
        relay_x = pass_on(gy, c, quarters[3], to_x)
        ax[1], ay[1] = pass_on(g, cm, first, to_x), pass_on(g, cm, first, to_y)
        bp[1], bm[1] = pass_on(gx, c, second, to_p), pass_on(gx, c, second, to_m)
        ax[2], ay[2] = pass_on(g, cp, first, to_x), pass_on(g, cp, first, to_y)
        bp[2], bm[2] = pass_on(gy, c, second, to_p), pass_on(gy, c, second, to_m)
        relay_p.wait_recv()
        relay_m.wait_recv()
        ax[3], ay[3] = pass_on(g, c2, first, to_x), pass_on(g, c2, first, to_y)
        relay_y.wait_recv()
        relay_x.wait_recv()
        bp[3], bm[3] = pass_on(gd, c, second, to_p), pass_on(gd, c, second, to_m)
        local.wait()
        last = [share(g, first)]
        columns, groups = (c, cm, cp, c2), (g, gx, gy, gd)
        for k in range(4):
            ax[k].wait_recv()
            last.append(pass_on(gx, columns[k], quarters[0], to_y))
            ay[k].wait_recv()
            last.append(pass_on(gy, columns[k], quarters[1], to_x))
            bp[k].wait_recv()
            last.append(pass_on(groups[k], cm, quarters[2], to_p))
            bm[k].wait_recv()
            last.append(pass_on(groups[k], cp, quarters[3], to_m))
        last.append(share(gx, first))
        last.append(share(gy, first))
        for k in range(4):
            for copy in last[1 + 4 * k : 5 + 4 * k]:
                copy.wait_recv()
            last.append(share(groups[k], second))
        last.append(share(gd, first))
        last[0].wait_recv()
        for copy in last[17:]:
            copy.wait_recv()
        for copy in started:
            copy.wait_send()

    return pl.pallas_call(
        kernel,
        out_shape=jax.ShapeDtypeStruct(shape, piece.dtype),
        in_specs=[pl.BlockSpec(memory_space=pl.ANY)],
        out_specs=pl.BlockSpec(memory_space=pl.ANY),
        scratch_shapes=[
            pltpu.SemaphoreType.DMA((64,)),
            pltpu.SemaphoreType.DMA((64,)),
            pltpu.SemaphoreType.DMA,
        ],
        compiler_params=pltpu.CompilerParams(collective_id=collective_id, has_side_effects=True),
    )(piece)


def gather_generator(x_piece):
    groups, n_row, n_col = (lax.axis_size(a) for a in ALL)
    rows, cols = x_piece.shape
    order = cols * n_col
    if (groups, n_row, n_col) != (4, 2, 4):
        whole = lax.all_gather(x_piece, ALL).reshape(groups, n_row, n_col, rows, cols)
        return whole.transpose(1, 0, 3, 2, 4).reshape(order, order)

    def lines(g, r, part):
        return pl.ds(pl.multiple_of((r * groups + g) * rows + part[0], 8), part[1])

    def place(ref, g, r, c, part):
        return ref.at[lines(g, r, part), pl.ds(pl.multiple_of(c * cols, 128), cols)]

    def band(ref, g, r, part):
        return ref.at[lines(g, r, part)]

    return wide_gather(x_piece, (order, order), place, band, 3)


def gather_expmap(slab):
    groups, n_row, n_col = (lax.axis_size(a) for a in ALL)
    rows, order = slab.shape
    if (groups, n_row, n_col) != (4, 2, 4):
        return lax.all_gather(slab, ALL, axis=0, tiled=True)

    def place(ref, g, r, c, part):
        return ref.at[(g * n_row + r) * n_col + c, pl.ds(*part)]

    def band(ref, g, r, part):
        return ref.at[pl.ds((g * n_row + r) * n_col, n_col), pl.ds(*part)]

    return wide_gather(slab, (order // rows, rows, order), place, band, 4).reshape(order, order)


def lookup_weights(bvec_index, weight_table):
    table_slots = jnp.arange(weight_table.shape[0], dtype=jnp.int32)
    return jnp.sum(
        jnp.where(table_slots[None, :] == bvec_index[:, None], weight_table[None, :], 0.0), axis=1
    )


def shards(m_matrices, bvec_index, weight_table, grad_prev, dir_prev):
    per_group = m_matrices.shape[0]
    local_rows = m_matrices.shape[2]
    local_cols = m_matrices.shape[3]
    groups, n_row, n_col = (lax.axis_size(a) for a in ALL)
    devices = groups * n_row * n_col
    order = local_rows * n_row
    group = lax.axis_index("bvec")
    row, col = lax.axis_index("row"), lax.axis_index("col")
    row_start = row * local_rows
    col_start = col * local_cols
    weight_all = lookup_weights(bvec_index, weight_table)
    weight_own = lax.dynamic_slice_in_dim(weight_all, group * per_group, per_group)
    row_ids = row_start + jnp.arange(local_rows, dtype=jnp.int32)
    col_ids = col_start + jnp.arange(local_cols, dtype=jnp.int32)
    on_diag = row_ids[:, None] == col_ids[None, :]
    own_diag = jnp.sum(jnp.where(on_diag, m_matrices, 0.0), axis=2)
    diag_parts = small_gather(own_diag.reshape(-1, 128), ("row", "col"), 0)
    diag_parts = diag_parts.reshape(n_row, n_col, per_group, 2, local_cols).sum(axis=0)
    diagonal = diag_parts.transpose(1, 2, 0, 3).reshape(per_group, 2, order)
    row_diag = lax.dynamic_slice_in_dim(diagonal, row_start, local_rows, 2)
    col_diag = lax.dynamic_slice_in_dim(diagonal, col_start, local_cols, 2)
    spread_own = (
        jnp.sum(weight_own[:, None] * (1.0 - diagonal[:, 0] ** 2 - diagonal[:, 1] ** 2)) / order
    )
    spread_term = jnp.where((row == 0) & (col == 0), spread_own, 0.0)
    differ = row_diag[:, :, :, None] - col_diag[:, :, None, :]
    weighted = 2.0 * weight_own[:, None, None] * jnp.sum(m_matrices * differ, axis=1)
    grad_part = jnp.sum(weighted, axis=0)
    grad_piece = lax.psum_scatter(grad_part, "bvec", scatter_dimension=0, tiled=True)
    piece_rows = local_rows // groups
    prev_piece = lax.dynamic_slice_in_dim(grad_prev, group * piece_rows, piece_rows, 0)
    dir_piece = lax.dynamic_slice_in_dim(dir_prev, group * piece_rows, piece_rows, 0)
    sums = jnp.stack(
        [
            spread_term,
            jnp.sum(grad_piece * grad_piece),
            jnp.sum(prev_piece * prev_piece),
            jnp.sum(grad_piece * dir_piece),
            jnp.sum(dir_piece * dir_piece),
        ]
    )
    sums = jnp.pad(sums[None, :], ((0, 7), (0, 128 - sums.shape[0])))
    totals = jnp.sum(small_gather(sums, ALL, 1), axis=0)[0]
    spread = totals[0]
    beta_factor = totals[1] / (1.0 + totals[2])
    dir_norm = jnp.maximum(
        totals[1] - 2.0 * beta_factor * totals[3] + beta_factor * beta_factor * totals[4], 0.0
    )
    scale = STEP_SCALE / jnp.sqrt(1.0 + dir_norm / order)
    x_piece = scale * (beta_factor * dir_piece - grad_piece)
    generator = gather_generator(x_piece)
    grad_in, _ = lax.optimization_barrier((grad_piece, generator[0, 0]))
    gradient = lax.all_gather(grad_in, "bvec", axis=0, tiled=True)
    direction = beta_factor * dir_prev - gradient

    slab = order // devices
    me = (group * n_row + row) * n_col + col
    slab_ids = me * slab + jnp.arange(slab, dtype=jnp.int32)
    eye_slab = (slab_ids[:, None] == jnp.arange(order, dtype=jnp.int32)[None, :]).astype(jnp.float32)
    iterate = eye_slab + lax.dynamic_slice_in_dim(generator, me * slab, slab, 0) / TAYLOR
    for divisor in range(TAYLOR - 1, 0, -1):
        iterate = eye_slab + product(iterate, generator) / divisor
    expmap = gather_expmap(iterate)
    exp_rows = lax.dynamic_slice_in_dim(expmap, row_start, local_rows, 0)
    exp_cols = lax.dynamic_slice_in_dim(expmap, col_start, local_cols, 0)
    flat = m_matrices.reshape(-1, local_cols)
    rotated = product(flat, exp_cols).reshape(per_group, 2, local_rows, order)
    trial_part = jnp.sum(exp_rows[None, None] * rotated, axis=2)
    trial_parts = small_gather(trial_part.reshape(-1, 128), ALL, 2)
    trial_diag = trial_parts.reshape(groups, n_row * n_col, per_group, 2, order).sum(axis=1)
    trial_diag = trial_diag.reshape(groups * per_group, 2, order)
    trial_spread = (
        jnp.sum(weight_all[:, None] * (1.0 - trial_diag[:, 0] ** 2 - trial_diag[:, 1] ** 2)) / order
    )
    return (spread, trial_spread, gradient, direction, trial_diag)


def solution(mesh):
    placed = (P("bvec", None, "row", "col"), P(), P(), P("row", "col"), P("row", "col"))
    return jax.shard_map(
        shards,
        mesh=mesh,
        in_specs=placed,
        out_specs=(P(), P(), P("row", "col"), P("row", "col"), P()),
        check_vma=False,
    )
```
